32 devices in a mesh: cfg: 2 (over x), seq: 16 (over z, y, core).
Axes of the slice: x: 2, y: 2, z: 4, core: 2. Of those that a mesh axis runs over, the one named last changes fastest.
Arguments:
- hidden: bfloat16 [2, 2048, 1920], P('cfg', 'seq'), may hold values from -6 to 6
- modulation: float32 [6, 1920], replicated, may hold values from -3 to 3
- w_qkv: bfloat16 [3, 1920, 1024], replicated, may hold values from -0.125 to 0.125
- q_gain: float32 [64], replicated, may hold values from 1 to 13, as said below
- k_gain: float32 [64], replicated, may hold values from 1 to 13, as said below
- w_out: bfloat16 [1024, 1920], replicated, may hold values from -0.1875 to 0.1875
- text_count: int32 [2], P('cfg'), may hold values from 1 to 226
- block_order: int32 [16], P('seq'), may hold values from 0 to 15, each once
Outputs:
- guided: float32 [2048, 1920], P('seq', 'cfg')
The draws below stay inside these ranges and needn't reach their ends.
Inputs may be any that keep to these rules, and one draw needn't show every extreme that they name: text_count[b] is how many of the 226 text positions of branch b (0 conditional, 1 unconditional) hold prompt tokens; keys at the other text positions are masked. Seq index j holds positions block_order[j] * 128 to block_order[j] * 128 + 127; every block appears once. `q_gain`: one gain for each of the 64 entries of a head, shared by all heads. `k_gain`: one gain for each of the 64 entries of a head, shared by all heads.
All inputs are finite; a program needn't handle non-finite values.
Results may differ from the reference program's by a relative error of at most 0.015.
The reference program's roundings to bfloat16 on the way (of `modded`, `key_bias`, `weights` and `attended`) count: a program that leaves them out, or rounds other values in their place, can miss the bound.
Values may be sent and summed in bfloat16 or wider, within the bound.
No kernel may reach another device: no remote copies, remote signals or barrier semaphores. Data moves between devices by JAX's collectives and lax.ppermute only.
A program may use at most 256 MiB of HBM per device.

```python
import math
import jax
import jax.numpy as jnp
from jax import lax

D = 1920
HEAD = 64
HEADS = 16
TOK_DEV = 128
TXT = 226
TOKENS = 2048
N_SEQ = 16


def norm_gain(key, member):
    large_count = 3
    large_low = 7.0
    large_high = 9.0
    ranking = jax.random.permutation(jax.random.fold_in(key, 9001), HEAD)
    chosen = ranking < large_count
    member_key = jax.random.fold_in(key, member)
    base_gain = jnp.exp(jax.random.uniform(jax.random.fold_in(member_key, 1), (HEAD,), jnp.float32, 0.0, math.log(2.2)))
    large_gain = jax.random.uniform(jax.random.fold_in(member_key, 2), (HEAD,), jnp.float32, large_low, large_high)
    return jnp.where(chosen, large_gain, base_gain).astype(jnp.float32)


def draw_q_gain(key, part):
    return norm_gain(key, 11)


def draw_k_gain(key, part):
    return norm_gain(key, 23)


def steps_of(rng, extent, cuts, smallest, high):
    loudness, own = 1.0, jax.random.fold_in(rng, 6)
    for dim, parts in cuts:
        heights = jnp.exp(jax.random.uniform(jax.random.fold_in(own, dim), (parts,), jnp.float32, smallest / len(cuts), high / len(cuts)))
        loudness = loudness * jnp.repeat(heights, extent[dim] // parts).reshape([-1 if axis == dim else 1 for axis in range(len(extent))])
    return loudness


def gaussian(key, dims, scale, most, split=(), kind=jnp.bfloat16):
    loudness = steps_of(key, dims, split, -0.22, 0.18) if split else 1.0
    drawn = jax.random.normal(key, dims, jnp.float32) * scale * loudness
    return jnp.minimum(jnp.maximum(drawn, -most), most).astype(kind)


def setup_inputs(seed: int = 0) -> dict:
    key_list = jax.random.split(jax.random.key(seed), 9)
    return {
        "hidden": gaussian(key_list[0], (2, TOKENS, D), 1.0, 6.0, ((0, 2), (1, 16))),
        "modulation": gaussian(key_list[1], (6, D), 0.5, 3.0, (), jnp.float32),
        "w_qkv": gaussian(key_list[2], (3, D, HEADS * HEAD), D ** -0.5, 0.125),
        "q_gain": draw_q_gain(jax.random.fold_in(key_list[8], 71), 0),
        "k_gain": draw_k_gain(jax.random.fold_in(key_list[8], 71), 0),
        "w_out": gaussian(key_list[5], (HEADS * HEAD, D), (HEADS * HEAD) ** -0.5, 0.1875),
        "text_count": jax.random.randint(key_list[6], (2,), 1, TXT + 1).astype(jnp.int32),
        "block_order": jax.random.permutation(key_list[7], N_SEQ).astype(jnp.int32),
    }


GUIDANCE = 6.0
EPSILON = 1e-05
MASKED = -1000000000.0

def layer_normal(values_in):
    average = lax.optimization_barrier(jnp.mean(values_in, axis=-1, keepdims=True))
    centred = values_in - average
    spread = lax.optimization_barrier(jnp.mean(centred * centred, axis=-1, keepdims=True))
    return centred * lax.rsqrt(spread + EPSILON)

def modulated(states, is_text, modulation):
    normed = layer_normal(states.astype(jnp.float32))
    shift = jnp.where(is_text[:, None], modulation[3][None, :], modulation[0][None, :])
    scale = jnp.where(is_text[:, None], modulation[4][None, :], modulation[1][None, :])
    return (normed * (1.0 + scale) + shift).astype(jnp.bfloat16)

def head_normal(projected, gain):
    rows = projected.shape[0]
    heads_view = projected.reshape(rows, HEADS, HEAD)
    return (layer_normal(heads_view) * gain).reshape(rows, HEADS * HEAD).astype(jnp.bfloat16)

def projections(states, is_text, modulation, w_qkv, q_gain, k_gain):
    modded = modulated(states, is_text, modulation)
    query = head_normal(jnp.dot(modded, w_qkv[0], preferred_element_type=jnp.float32), q_gain)
    keys = head_normal(jnp.dot(modded, w_qkv[1], preferred_element_type=jnp.float32), k_gain)
    values = jnp.dot(modded, w_qkv[2], preferred_element_type=jnp.float32).astype(jnp.bfloat16)
    return (query, keys, values)

def attend_block(query_block, key_heads, value_heads, bias_wide):
    rows = query_block.shape[0]
    query_heads = query_block.astype(jnp.float32).reshape(rows, HEADS, HEAD)
    scores = jnp.einsum('qhd,khd->hqk', query_heads, key_heads) * HEAD ** (-0.5) + bias_wide[None, None, :]
    highest = lax.optimization_barrier(jnp.max(scores, axis=-1, keepdims=True))
    expo = jnp.exp(scores - highest)
    total = lax.optimization_barrier(jnp.sum(expo, axis=-1))
    weights = expo.astype(jnp.bfloat16).astype(jnp.float32)
    numer = jnp.einsum('hqk,khd->qhd', weights, value_heads)
    return (numer / total.T[:, :, None]).reshape(rows, HEADS * HEAD).astype(jnp.bfloat16)

def reference(hidden, modulation, w_qkv, q_gain, k_gain, w_out, text_count, block_order):
    within = jnp.arange(TOK_DEV, dtype=jnp.int32)
    position = (block_order[:, None].astype(jnp.int32) * TOK_DEV + within[None, :]).reshape(TOKENS)
    is_text = position < TXT
    gate = jnp.where(is_text[:, None], modulation[5][None, :], modulation[2][None, :])
    query_rows = 512 if TOKENS % 512 == 0 else TOKENS

    def one_branch(states, count):
        keep = jnp.logical_or(position >= TXT, position < count)
        key_bias = jnp.where(keep, 0.0, MASKED).astype(jnp.bfloat16)
        query, keys, values = projections(states, is_text, modulation, w_qkv, q_gain, k_gain)
        key_heads = keys.astype(jnp.float32).reshape(TOKENS, HEADS, HEAD)
        value_heads = values.astype(jnp.float32).reshape(TOKENS, HEADS, HEAD)
        bias_wide = key_bias.astype(jnp.float32)
        query_blocks = query.reshape(TOKENS // query_rows, query_rows, HEADS * HEAD)

        def attend(block):
            return attend_block(block, key_heads, value_heads, bias_wide)
        attended = lax.map(attend, query_blocks).reshape(TOKENS, HEADS * HEAD)
        return gate * jnp.dot(attended, w_out, preferred_element_type=jnp.float32)
    cond = one_branch(hidden[0], text_count[0])
    uncond = one_branch(hidden[1], text_count[1])
    return uncond + GUIDANCE * (cond - uncond)
```

```python
import functools

import jax
import jax.numpy as jnp
from jax import lax
from jax.experimental import pallas as pl
from jax.experimental.pallas import tpu as pltpu
from jax.sharding import PartitionSpec as P

TXT = 226
GUIDANCE = 6.0
EPSILON = 1e-05
MASKED = -1000000000.0
WAYS = 4
LANES = 128
EXTRA = 16


def text_rows(block, rows):
    within = lax.broadcasted_iota(jnp.int32, (rows, 1), 0)
    return block * rows + within < TXT


def modulate(block, states, modulation_ref):
    average = jnp.mean(states, axis=-1, keepdims=True)
    centred = states - average
    spread = jnp.mean(centred * centred, axis=-1, keepdims=True)
    normed = centred * lax.rsqrt(spread + EPSILON)
    is_text = text_rows(block, states.shape[0])
    table = modulation_ref[...]
    shift = jnp.where(is_text, table[3:4, :], table[0:1, :])
    scale = jnp.where(is_text, table[4:5, :], table[1:2, :])
    return (normed * (1.0 + scale) + shift).astype(jnp.bfloat16)


def head_normal(tile, gain, head):
    lane = lax.broadcasted_iota(jnp.int32, (1, LANES), 1)

    def average(x):
        mean = jnp.zeros(x.shape, jnp.float32)
        for first in range(0, LANES, head):
            inside = (lane >= first) & (lane < first + head)
            total = jnp.sum(jnp.where(inside, x, 0.0), axis=-1, keepdims=True)
            mean = jnp.where(inside, total * (1.0 / head), mean)
        return mean

    centred = tile - average(tile)
    return centred * lax.rsqrt(average(centred * centred) + EPSILON) * gain


def wide(gain):
    return jnp.concatenate([gain] * (LANES // gain.shape[1]), axis=-1)


def key_value_kernel(block_ref, count_ref, hidden_ref, modulation_ref, w_ref, gain_ref, *refs, head, groups):
    slots, (modded_ref, w_all, sems) = refs[:WAYS], refs[WAYS:]
    copies = [pltpu.make_async_copy(w_ref.at[1 + i], w_all.at[i], sems.at[i]) for i in range(2)]
    for copy in copies:
        copy.start()
    block = block_ref[0]
    modded_ref[...] = modulate(block, hidden_ref[...].astype(jnp.float32), modulation_ref)
    rows = modded_ref.shape[0]
    width = w_all.shape[2] // WAYS
    gain = wide(gain_ref[...])
    way = lax.axis_index("seq") // groups
    position = block * rows + lax.broadcasted_iota(jnp.int32, (EXTRA, rows), 1)
    keep = (position >= TXT) | (position < count_ref[0])
    bias = jnp.where(keep, 0.0, MASKED).astype(jnp.bfloat16)
    starts = [pl.multiple_of((way ^ slot) * width, width) for slot in range(WAYS)]
    copies[0].wait()
    for slot in range(WAYS):
        w = w_all[0, :, pl.ds(starts[slot], width)]
        keys = jnp.dot(modded_ref[...], w, preferred_element_type=jnp.float32)
        for tile in range(width // LANES):
            normed = head_normal(keys[:, tile * LANES : (tile + 1) * LANES], gain, head)
            slots[slot][tile * rows : (tile + 1) * rows, :] = normed.astype(jnp.bfloat16)
        at = rows * (width // LANES)
        slots[slot][at : at + EXTRA, :] = bias
    copies[1].wait()
    for slot in range(WAYS):
        w = w_all[1, :, pl.ds(starts[slot], width)]
        values = jnp.dot(modded_ref[...], w, preferred_element_type=jnp.float32)
        slots[slot][at + EXTRA :, :] = values.T.astype(jnp.bfloat16)


def query_kernel(modded_ref, w_ref, gain_ref, *refs, head, groups):
    slots, (w_all, sem) = refs[:WAYS], refs[WAYS:]
    copy = pltpu.make_async_copy(w_ref.at[0], w_all, sem)
    copy.start()
    width = w_all.shape[1] // WAYS
    gain = wide(gain_ref[...])
    way = lax.axis_index("seq") // groups
    copy.wait()
    for slot in range(WAYS):
        start = pl.multiple_of((way ^ slot) * width, width)
        query = jnp.dot(modded_ref[...], w_all[:, pl.ds(start, width)], preferred_element_type=jnp.float32)
        for tile in range(width // LANES):
            at = slice(tile * LANES, (tile + 1) * LANES)
            normed = head_normal(query[:, at], gain, head).astype(jnp.bfloat16)
            slots[slot][:, at] = normed * jnp.asarray(head ** (-0.5), jnp.bfloat16)


def attention_kernel(*refs, held, head):
    queries, refs = refs[:WAYS], refs[WAYS:]
    pieces, refs = refs[:held], refs[held:]
    outs, (k_all, v_all, b_all, q_all, o_all) = refs[:WAYS], refs[WAYS:]
    rows, width = queries[0].shape
    heads = width // head
    tiles = width // LANES
    deep = head + EXTRA
    size = tiles * rows + EXTRA + width
    each = pieces[0].shape[0] // size
    biases = []
    for g in range(held):
        for p in range(each):
            to, at = (g * each + p) * rows, p * size
            for tile in range(tiles):
                k_all[to : to + rows, tile * LANES : (tile + 1) * LANES] = pieces[g][at + tile * rows : at + (tile + 1) * rows, :]
            at += tiles * rows
            biases.append(pieces[g][at : at + EXTRA, :].astype(jnp.float32)[0:1, :])
            at += EXTRA
            for h in range(heads):
                v_all[h, :head, to : to + rows] = pieces[g][at + h * head : at + (h + 1) * head, :]
    for h in range(heads):
        v_all[h, head:, :] = jnp.ones((EXTRA, v_all.shape[2]), jnp.bfloat16)
    for first in range(0, len(biases), LANES):
        some = biases[first : first + LANES]
        fill = [jnp.zeros((LANES - len(some), LANES), jnp.float32)] if len(some) < LANES else []
        columns = jnp.concatenate(some + fill, axis=0).T
        for i in range(len(some)):
            to = (first + i) * rows
            b_all[to : to + rows, :] = jnp.broadcast_to(columns[:, i : i + 1], (rows, LANES))
    for slot in range(WAYS):
        q_all[slot * rows : (slot + 1) * rows, :] = queries[slot][...]
    lane = lax.broadcasted_iota(jnp.int32, (1, width), 1)
    span = 2 * rows

    def one_block(index, _):
        query = q_all[pl.ds(pl.multiple_of(index * span, span), span), :]
        columns = []
        for h in range(heads):
            inside = (lane >= h * head) & (lane < (h + 1) * head)
            masked = jnp.where(inside, query, jnp.zeros_like(query))
            scores = lax.dot_general(k_all[...], masked, (((1,), (1,)), ((), ())), preferred_element_type=jnp.float32)
            bias = b_all[...]
            scores = scores + jnp.concatenate([bias] * (span // LANES), axis=-1)
            expo = jnp.exp(scores - jnp.max(scores, axis=0, keepdims=True)).astype(jnp.bfloat16)
            numer = jnp.dot(v_all[h], expo, preferred_element_type=jnp.float32)
            columns.append(numer[:head, :] / numer[head : head + 1, :])
        o_all[index] = jnp.concatenate(columns, axis=0)
        return 0

    lax.fori_loop(0, WAYS // 2, one_block, 0)
    for slot in range(WAYS):
        at = (slot % 2) * rows
        outs[slot][...] = o_all[slot // 2, :, at : at + rows].T.astype(jnp.bfloat16)


def project(pieces_ref, w_ref, way, start, span):
    width = pieces_ref.shape[1]
    rows = pieces_ref.shape[0] // WAYS
    total = jnp.zeros((rows, span), jnp.float32)
    for slot in range(WAYS):
        at = pl.multiple_of((way ^ slot) * width, width)
        w = w_ref[pl.ds(at, width), pl.ds(start, span)]
        total += jnp.dot(pieces_ref[slot * rows : (slot + 1) * rows, :], w, preferred_element_type=jnp.float32)
    return total


def half_of(total):
    half = total // 2
    spare = half % LANES
    span = half + spare
    start = pl.multiple_of(lax.axis_index("cfg") * (half - spare), LANES)
    return half, spare, span, start


def own_kernel(pieces_ref, w_ref, out_ref, *, groups):
    _, _, span, start = half_of(w_ref.shape[1])
    out_ref[...] = project(pieces_ref, w_ref, lax.axis_index("seq") // groups, start, span)


def final_kernel(block_ref, pieces_ref, own_ref, w_ref, modulation_ref, out_ref, *, groups):
    half, spare, span, start = half_of(w_ref.shape[1])
    total = project(pieces_ref, w_ref, lax.axis_index("seq") // groups, start, span)
    is_text = text_rows(block_ref[0], total.shape[0])
    table = modulation_ref[:, pl.ds(start, span)]
    gate = jnp.where(is_text, table[5:6, :], table[2:3, :])
    other = gate * total
    own = gate * own_ref[...]
    is_first = lax.axis_index("cfg") == 0
    cond = jnp.where(is_first, own, other)
    uncond = jnp.where(is_first, other, own)
    guided = (uncond + GUIDANCE * (cond - uncond)).T
    out_ref[...] = jnp.where(is_first, guided[:half, :], guided[spare:, :])


def shards(hidden, modulation, w_qkv, q_gain, k_gain, w_out, text_count, block_order):
    states = hidden[0]
    rows, features = states.shape
    head = q_gain.shape[0]
    inner = w_qkv.shape[2]
    width = inner // WAYS
    count = lax.axis_size("seq")
    groups = count // WAYS
    bf16 = jnp.bfloat16
    smem = pl.BlockSpec(memory_space=pltpu.SMEM)
    vmem = pl.BlockSpec(memory_space=pltpu.VMEM)
    hbm = pl.BlockSpec(memory_space=pl.ANY)

    def exchange(block, bits):
        return lax.ppermute(block, "seq", [(i, i ^ bits) for i in range(count)])

    def spread(slots):
        far = {s: exchange(slots[s], s * groups) for s in reversed(range(1, WAYS))}
        return [slots[0]] + [far[s] for s in range(1, WAYS)]

    size = (width // LANES) * rows + EXTRA + width
    kv_piece = jax.ShapeDtypeStruct((size, LANES), bf16)
    piece = jax.ShapeDtypeStruct((rows, width), bf16)
    *kv_slots, modded = pl.pallas_call(
        functools.partial(key_value_kernel, head=head, groups=groups),
        in_specs=[smem, smem, vmem, vmem, hbm, vmem],
        out_shape=[kv_piece] * WAYS + [jax.ShapeDtypeStruct((rows, features), bf16)],
        scratch_shapes=[pltpu.VMEM((2, features, inner), bf16), pltpu.SemaphoreType.DMA((2,))],
    )(block_order, text_count, states, modulation, w_qkv, k_gain[None, :])
    kv = spread(kv_slots)
    q_slots = pl.pallas_call(
        functools.partial(query_kernel, head=head, groups=groups),
        in_specs=[vmem, hbm, vmem],
        out_shape=[piece] * WAYS,
        scratch_shapes=[pltpu.VMEM((features, inner), bf16), pltpu.SemaphoreType.DMA],
    )(modded, w_qkv, q_gain[None, :])
    queries = spread(q_slots)
    held = [jnp.concatenate(kv[i : i + 2], axis=0) for i in range(0, WAYS, 2)]
    bit = groups // 2
    while bit:
        held = held + [exchange(x, bit) for x in held]
        bit //= 2

    keys = count * rows
    o_slots = pl.pallas_call(
        functools.partial(attention_kernel, held=len(held), head=head),
        in_specs=[vmem] * (WAYS + len(held)),
        out_shape=[piece] * WAYS,
        scratch_shapes=[
            pltpu.VMEM((keys, width), bf16),
            pltpu.VMEM((width // head, head + EXTRA, keys), bf16),
            pltpu.VMEM((keys, LANES), jnp.float32),
            pltpu.VMEM((WAYS * rows, width), bf16),
            pltpu.VMEM((WAYS // 2, width, 2 * rows), jnp.float32),
        ],
    )(*queries, *held)
    attended = jnp.concatenate(spread(o_slots), axis=0)
    cfg_count = lax.axis_size("cfg")
    partner = lax.ppermute(attended, "cfg", [(i, i ^ 1) for i in range(cfg_count)])

    half = w_out.shape[1] // 2
    span = half + half % LANES
    own = pl.pallas_call(
        functools.partial(own_kernel, groups=groups),
        in_specs=[vmem] * 2,
        out_shape=jax.ShapeDtypeStruct((rows, span), jnp.float32),
    )(attended, w_out)
    guided = pl.pallas_call(
        functools.partial(final_kernel, groups=groups),
        in_specs=[smem] + [vmem] * 4,
        out_shape=jax.ShapeDtypeStruct((half, rows), jnp.float32),
    )(block_order, partner, own, w_out, modulation)
    return guided.T


def solution(mesh):
    in_specs = (P("cfg", "seq", None), P(), P(), P(), P(), P(), P("cfg"), P("seq"))
    out_specs = P("seq", "cfg")
    return jax.shard_map(shards, mesh=mesh, in_specs=in_specs, out_specs=out_specs, check_vma=False)
```

```python
import functools

import jax
import jax.numpy as jnp
from jax import lax
from jax.experimental import pallas as pl
from jax.experimental.pallas import tpu as pltpu
from jax.sharding import PartitionSpec as P


TXT = 226
GUIDANCE = 6.0
EPSILON = 1e-05
MASKED = -1000000000.0
WAYS = 4
LANES = 128
EXTRA = 16


def text_rows(block, rows):
    within = lax.broadcasted_iota(jnp.int32, (rows, 1), 0)
    return block * rows + within < TXT


def modulate(block, states, modulation_ref):
    average = jnp.mean(states, axis=-1, keepdims=True)
    centred = states - average
    spread = jnp.mean(centred * centred, axis=-1, keepdims=True)
    normed = centred * lax.rsqrt(spread + EPSILON)
    is_text = text_rows(block, states.shape[0])
    table = modulation_ref[...]
    shift = jnp.where(is_text, table[3:4, :], table[0:1, :])
    scale = jnp.where(is_text, table[4:5, :], table[1:2, :])
    return (normed * (1.0 + scale) + shift).astype(jnp.bfloat16)


def head_normal(tile, gain, head):
    lane = lax.broadcasted_iota(jnp.int32, (1, LANES), 1)

    def average(x):
        mean = jnp.zeros(x.shape, jnp.float32)
        for first in range(0, LANES, head):
            inside = (lane >= first) & (lane < first + head)
            total = jnp.sum(jnp.where(inside, x, 0.0), axis=-1, keepdims=True)
            mean = jnp.where(inside, total * (1.0 / head), mean)
        return mean

    centred = tile - average(tile)
    return centred * lax.rsqrt(average(centred * centred) + EPSILON) * gain


def wide(gain):
    return jnp.concatenate([gain] * (LANES // gain.shape[1]), axis=-1)


def key_value_kernel(block_ref, count_ref, hidden_ref, modulation_ref, w_ref, gain_ref, *refs, head, groups):
    slots, (modded_ref, states, table, w_all, sems) = refs[:WAYS], refs[WAYS:]
    first = [
        pltpu.make_async_copy(hidden_ref, states, sems.at[2]),
        pltpu.make_async_copy(modulation_ref, table, sems.at[3]),
    ]
    copies = [pltpu.make_async_copy(w_ref.at[1 + i], w_all.at[i], sems.at[i]) for i in range(2)]
    for copy in first + copies:
        copy.start()
    for copy in first:
        copy.wait()
    block = block_ref[0]
    modded_ref[...] = modulate(block, states[...].astype(jnp.float32), table)
    rows = modded_ref.shape[0]
    width = w_all.shape[2] // WAYS
    gain = wide(gain_ref[...])
    way = lax.axis_index("seq") // groups
    position = block * rows + lax.broadcasted_iota(jnp.int32, (EXTRA, rows), 1)
    keep = (position >= TXT) | (position < count_ref[0])
    bias = jnp.where(keep, 0.0, MASKED).astype(jnp.bfloat16)
    starts = [pl.multiple_of((way ^ slot) * width, width) for slot in range(WAYS)]
    copies[0].wait()
    for slot in range(WAYS):
        w = w_all[0, :, pl.ds(starts[slot], width)]
        keys = jnp.dot(modded_ref[...], w, preferred_element_type=jnp.float32)
        for tile in range(width // LANES):
            normed = head_normal(keys[:, tile * LANES : (tile + 1) * LANES], gain, head)
            slots[slot][tile * rows : (tile + 1) * rows, :] = normed.astype(jnp.bfloat16)
        at = rows * (width // LANES)
        slots[slot][at : at + EXTRA, :] = bias
    copies[1].wait()
    for slot in range(WAYS):
        w = w_all[1, :, pl.ds(starts[slot], width)]
        values = jnp.dot(modded_ref[...], w, preferred_element_type=jnp.float32)
        slots[slot][at + EXTRA :, :] = values.T.astype(jnp.bfloat16)


def query_kernel(modded_ref, w_ref, gain_ref, *refs, head, groups):
    slots, (w_all, sem) = refs[:WAYS], refs[WAYS:]
    copy = pltpu.make_async_copy(w_ref.at[0], w_all, sem)
    copy.start()
    width = w_all.shape[1] // WAYS
    gain = wide(gain_ref[...])
    way = lax.axis_index("seq") // groups
    copy.wait()
    for slot in range(WAYS):
        start = pl.multiple_of((way ^ slot) * width, width)
        query = jnp.dot(modded_ref[...], w_all[:, pl.ds(start, width)], preferred_element_type=jnp.float32)
        for tile in range(width // LANES):
            at = slice(tile * LANES, (tile + 1) * LANES)
            normed = head_normal(query[:, at], gain, head).astype(jnp.bfloat16)
            slots[slot][:, at] = normed * jnp.asarray(head ** (-0.5), jnp.bfloat16)


def attention_kernel(*refs, held, head):
    queries, refs = refs[:WAYS], refs[WAYS:]
    pieces, refs = refs[:held], refs[held:]
    outs, (k_all, v_all, b_all, q_all, o_all) = refs[:WAYS], refs[WAYS:]
    rows, width = queries[0].shape
    heads = width // head
    tiles = width // LANES
    size = tiles * rows + EXTRA + width
    biases = []
    for g in range(held):
        for p in range(pieces[g].shape[0] // size):
            to, at = len(biases) * rows, p * size
            for tile in range(tiles):
                k_all[to : to + rows, tile * LANES : (tile + 1) * LANES] = pieces[g][at + tile * rows : at + (tile + 1) * rows, :]
            at += tiles * rows
            biases.append(pieces[g][at : at + EXTRA, :].astype(jnp.float32)[0:1, :])
            at += EXTRA
            for h in range(heads):
                v_all[h, :head, to : to + rows] = pieces[g][at + h * head : at + (h + 1) * head, :]
    for h in range(heads):
        v_all[h, head:, :] = jnp.ones((EXTRA, v_all.shape[2]), jnp.bfloat16)
    for first in range(0, len(biases), LANES):
        some = biases[first : first + LANES]
        fill = [jnp.zeros((LANES - len(some), LANES), jnp.float32)] if len(some) < LANES else []
        columns = jnp.concatenate(some + fill, axis=0).T
        for i in range(len(some)):
            to = (first + i) * rows
            b_all[to : to + rows, :] = jnp.broadcast_to(columns[:, i : i + 1], (rows, LANES))
    for slot in range(WAYS):
        q_all[slot * rows : (slot + 1) * rows, :] = queries[slot][...]
    lane = lax.broadcasted_iota(jnp.int32, (1, width), 1)
    span = 2 * rows

    def one_block(index, _):
        query = q_all[pl.ds(pl.multiple_of(index * span, span), span), :]
        columns = []
        for h in range(heads):
            inside = (lane >= h * head) & (lane < (h + 1) * head)
            masked = jnp.where(inside, query, jnp.zeros_like(query))
            scores = lax.dot_general(k_all[...], masked, (((1,), (1,)), ((), ())), preferred_element_type=jnp.float32)
            bias = b_all[...]
            scores = scores + jnp.concatenate([bias] * (span // LANES), axis=-1)
            expo = jnp.exp(scores - jnp.max(scores, axis=0, keepdims=True)).astype(jnp.bfloat16)
            numer = jnp.dot(v_all[h], expo, preferred_element_type=jnp.float32)
            columns.append(numer[:head, :] / numer[head : head + 1, :])
        o_all[index] = jnp.concatenate(columns, axis=0)
        return 0

    lax.fori_loop(0, WAYS // 2, one_block, 0)
    for slot in range(WAYS):
        at = (slot % 2) * rows
        outs[slot][...] = o_all[slot // 2, :, at : at + rows].T.astype(jnp.bfloat16)


def project(pieces_ref, w_ref, way, start, span):
    width = pieces_ref.shape[1]
    rows = pieces_ref.shape[0] // WAYS
    total = jnp.zeros((rows, span), jnp.float32)
    for slot in range(WAYS):
        at = pl.multiple_of((way ^ slot) * width, width)
        w = w_ref[pl.ds(at, width), pl.ds(start, span)]
        total += jnp.dot(pieces_ref[slot * rows : (slot + 1) * rows, :], w, preferred_element_type=jnp.float32)
    return total


def half_of(half):
    spare = half % LANES
    span = half + spare
    return spare, span, pl.multiple_of(lax.axis_index("cfg") * (half - spare), LANES)


def fetch_kernel(w_ref, out_ref, sem):
    _, span, start = half_of(w_ref.shape[1] // 2)
    copy = pltpu.make_async_copy(w_ref.at[:, pl.ds(start, span)], out_ref, sem)
    copy.start()
    copy.wait()


def project(pieces_ref, w_ref, way):
    width = pieces_ref.shape[1]
    rows = pieces_ref.shape[0] // WAYS
    total = jnp.zeros((rows, w_ref.shape[1]), jnp.float32)
    for slot in range(WAYS):
        w = w_ref[pl.ds(pl.multiple_of((way ^ slot) * width, width), width), :]
        total += jnp.dot(pieces_ref[slot * rows : (slot + 1) * rows, :], w, preferred_element_type=jnp.float32)
    return total


def own_kernel(pieces_ref, w_ref, out_ref, *, groups):
    out_ref[...] = project(pieces_ref, w_ref, lax.axis_index("seq") // groups)


def final_kernel(block_ref, pieces_ref, own_ref, w_ref, modulation_ref, out_ref, *, groups, half):
    spare, span, start = half_of(half)
    total = project(pieces_ref, w_ref, lax.axis_index("seq") // groups)
    is_text = text_rows(block_ref[0], total.shape[0])
    table = modulation_ref[:, pl.ds(start, span)]
    gate = jnp.where(is_text, table[5:6, :], table[2:3, :])
    other = gate * total
    own = gate * own_ref[...]
    is_first = lax.axis_index("cfg") == 0
    cond = jnp.where(is_first, own, other)
    uncond = jnp.where(is_first, other, own)
    guided = (uncond + GUIDANCE * (cond - uncond)).T
    out_ref[...] = jnp.where(is_first, guided[:half, :], guided[spare:, :])


def block(hidden, modulation, w_qkv, q_gain, k_gain, w_out, text_count, block_order):
    states = hidden[0]
    rows, features = states.shape
    head = q_gain.shape[0]
    inner = w_qkv.shape[2]
    width = inner // WAYS
    count = lax.axis_size("seq")
    groups = count // WAYS
    bf16 = jnp.bfloat16
    smem = pl.BlockSpec(memory_space=pltpu.SMEM)
    vmem = pl.BlockSpec(memory_space=pltpu.VMEM)
    hbm = pl.BlockSpec(memory_space=pl.ANY)
    held_in = functools.partial(pltpu.with_memory_space_constraint, memory_space=pltpu.VMEM)

    def exchange(x, bits):
        return lax.ppermute(x, "seq", [(i, i ^ bits) for i in range(count)])

    def spread(slots):
        far = {s: exchange(slots[s], s * groups) for s in reversed(range(1, WAYS))}
        return [slots[0]] + [far[s] for s in range(1, WAYS)]

    size = (width // LANES) * rows + EXTRA + width
    kv_piece = jax.ShapeDtypeStruct((size, LANES), bf16)
    piece = jax.ShapeDtypeStruct((rows, width), bf16)
    *kv_slots, modded = pl.pallas_call(
        functools.partial(key_value_kernel, head=head, groups=groups),
        in_specs=[smem, smem, hbm, hbm, hbm, vmem],
        out_shape=[kv_piece] * WAYS + [pltpu.VMEM((rows, features), bf16)],
        scratch_shapes=[
            pltpu.VMEM((rows, features), bf16),
            pltpu.VMEM(modulation.shape, jnp.float32),
            pltpu.VMEM((2, features, inner), bf16),
            pltpu.SemaphoreType.DMA((4,)),
        ],
    )(block_order, text_count, states, modulation, w_qkv, k_gain[None, :])
    kv = spread(kv_slots)
    q_slots = pl.pallas_call(
        functools.partial(query_kernel, head=head, groups=groups),
        in_specs=[vmem, hbm, vmem],
        out_shape=[piece] * WAYS,
        scratch_shapes=[pltpu.VMEM((features, inner), bf16), pltpu.SemaphoreType.DMA],
    )(held_in(modded), w_qkv, q_gain[None, :])
    queries = spread(q_slots)
    half = w_out.shape[1] // 2
    span = half + half % LANES
    w_half = pl.pallas_call(
        fetch_kernel,
        in_specs=[hbm],
        out_shape=pltpu.VMEM((inner, span), bf16),
        scratch_shapes=[pltpu.SemaphoreType.DMA],
    )(w_out)
    held = [kv[0], kv[1], jnp.concatenate(kv[2:], axis=0)]
    bit = groups // 2
    while bit:
        held = held + [exchange(x, bit) for x in held]
        bit //= 2

    keys = count * rows
    o_slots = pl.pallas_call(
        functools.partial(attention_kernel, held=len(held), head=head),
        in_specs=[vmem] * (WAYS + len(held)),
        out_shape=[piece] * WAYS,
        scratch_shapes=[
            pltpu.VMEM((keys, width), bf16),
            pltpu.VMEM((width // head, head + EXTRA, keys), bf16),
            pltpu.VMEM((keys, LANES), jnp.float32),
            pltpu.VMEM((WAYS * rows, width), bf16),
            pltpu.VMEM((WAYS // 2, width, 2 * rows), jnp.float32),
        ],
    )(*queries, *held)
    attended = jnp.concatenate(spread(o_slots), axis=0)
    cfg_count = lax.axis_size("cfg")
    partner = lax.ppermute(attended, "cfg", [(i, i ^ 1) for i in range(cfg_count)])
    own = pl.pallas_call(
        functools.partial(own_kernel, groups=groups),
        in_specs=[vmem] * 2,
        out_shape=pltpu.VMEM((rows, span), jnp.float32),
    )(attended, held_in(w_half))
    guided = pl.pallas_call(
        functools.partial(final_kernel, groups=groups, half=half),
        in_specs=[smem] + [vmem] * 4,
        out_shape=jax.ShapeDtypeStruct((half, rows), jnp.float32),
    )(block_order, partner, held_in(own), held_in(w_half), modulation)
    return guided.T


def solution(mesh):
    in_specs = (P("cfg", "seq", None), P(), P(), P(), P(), P(), P("cfg"), P("seq"))
    out_specs = P("seq", "cfg")
    return jax.shard_map(block, mesh=mesh, in_specs=in_specs, out_specs=out_specs, check_vma=False)
```

```python
import functools

import jax
import jax.numpy as jnp
from jax import lax
from jax.experimental import pallas as pl
from jax.experimental.pallas import tpu as pltpu
from jax.sharding import PartitionSpec as P


TXT = 226
GUIDANCE = 6.0
EPSILON = 1e-05
MASKED = -1000000000.0
WAYS = 4
LANES = 128
EXTRA = 16


def text_rows(block, rows):
    within = lax.broadcasted_iota(jnp.int32, (rows, 1), 0)
    return block * rows + within < TXT


def modulate(block, states, modulation_ref):
    average = jnp.mean(states, axis=-1, keepdims=True)
    centred = states - average
    spread = jnp.mean(centred * centred, axis=-1, keepdims=True)
    normed = centred * lax.rsqrt(spread + EPSILON)
    is_text = text_rows(block, states.shape[0])
    table = modulation_ref[...]
    shift = jnp.where(is_text, table[3:4, :], table[0:1, :])
    scale = jnp.where(is_text, table[4:5, :], table[1:2, :])
    return (normed * (1.0 + scale) + shift).astype(jnp.bfloat16)


def head_normal(tile, gain, head):
    lane = lax.broadcasted_iota(jnp.int32, (1, LANES), 1)

    def average(x):
        mean = jnp.zeros(x.shape, jnp.float32)
        for first in range(0, LANES, head):
            inside = (lane >= first) & (lane < first + head)
            total = jnp.sum(jnp.where(inside, x, 0.0), axis=-1, keepdims=True)
            mean = jnp.where(inside, total * (1.0 / head), mean)
        return mean

    centred = tile - average(tile)
    return centred * lax.rsqrt(average(centred * centred) + EPSILON) * gain


def wide(gain):
    return jnp.concatenate([gain] * (LANES // gain.shape[1]), axis=-1)


def key_value_kernel(block_ref, count_ref, hidden_ref, modulation_ref, w_ref, gain_ref, *refs, head, groups):
    slots, (modded_ref, states, table, w_all, sems) = refs[:WAYS], refs[WAYS:]
    first = [
        pltpu.make_async_copy(hidden_ref, states, sems.at[2]),
        pltpu.make_async_copy(modulation_ref, table, sems.at[3]),
    ]
    copies = [pltpu.make_async_copy(w_ref.at[1 + i], w_all.at[i], sems.at[i]) for i in range(2)]
    for copy in first + copies:
        copy.start()
    for copy in first:
        copy.wait()
    block = block_ref[0]
    modded_ref[...] = modulate(block, states[...].astype(jnp.float32), table)
    rows = modded_ref.shape[0]
    width = w_all.shape[2] // WAYS
    gain = wide(gain_ref[...])
    way = lax.axis_index("seq") // groups
    position = block * rows + lax.broadcasted_iota(jnp.int32, (EXTRA, rows), 1)
    keep = (position >= TXT) | (position < count_ref[0])
    bias = jnp.where(keep, 0.0, MASKED).astype(jnp.bfloat16)
    starts = [pl.multiple_of((way ^ slot) * width, width) for slot in range(WAYS)]
    copies[0].wait()
    for slot in range(WAYS):
        w = w_all[0, :, pl.ds(starts[slot], width)]
        keys = jnp.dot(modded_ref[...], w, preferred_element_type=jnp.float32)
        for tile in range(width // LANES):
            normed = head_normal(keys[:, tile * LANES : (tile + 1) * LANES], gain, head)
            slots[slot][tile * rows : (tile + 1) * rows, :] = normed.astype(jnp.bfloat16)
        at = rows * (width // LANES)
        slots[slot][at : at + EXTRA, :] = bias
    copies[1].wait()
    for slot in range(WAYS):
        w = w_all[1, :, pl.ds(starts[slot], width)]
        values = jnp.dot(modded_ref[...], w, preferred_element_type=jnp.float32)
        slots[slot][at + EXTRA :, :] = values.T.astype(jnp.bfloat16)


def query_kernel(modded_ref, w_ref, gain_ref, *refs, head, groups):
    slots, (w_all, sem) = refs[:WAYS], refs[WAYS:]
    copy = pltpu.make_async_copy(w_ref.at[0], w_all, sem)
    copy.start()
    width = w_all.shape[1] // WAYS
    gain = wide(gain_ref[...])
    way = lax.axis_index("seq") // groups
    copy.wait()
    for slot in range(WAYS):
        start = pl.multiple_of((way ^ slot) * width, width)
        query = jnp.dot(modded_ref[...], w_all[:, pl.ds(start, width)], preferred_element_type=jnp.float32)
        for tile in range(width // LANES):
            at = slice(tile * LANES, (tile + 1) * LANES)
            normed = head_normal(query[:, at], gain, head).astype(jnp.bfloat16)
            slots[slot][:, at] = normed * jnp.asarray(head ** (-0.5), jnp.bfloat16)


def attention_kernel(*refs, held, head, earlier):
    queries, refs = refs[:WAYS], refs[WAYS:]
    pieces, refs = refs[:held], refs[held:]
    if earlier:
        before, *outs, k_all, v_all, b_all, q_all, o_all = refs
    else:
        o_all, k_all, v_all, b_all, q_all = refs
    rows, width = queries[0].shape
    heads = width // head
    tiles = width // LANES
    deep = head + EXTRA
    size = tiles * rows + EXTRA + width
    biases = []
    for g in range(held):
        for p in range(pieces[g].shape[0] // size):
            to, at = len(biases) * rows, p * size
            for tile in range(tiles):
                k_all[to : to + rows, tile * LANES : (tile + 1) * LANES] = pieces[g][at + tile * rows : at + (tile + 1) * rows, :]
            at += tiles * rows
            biases.append(pieces[g][at : at + EXTRA, :].astype(jnp.float32)[0:1, :])
            at += EXTRA
            for h in range(heads):
                v_all[h, :head, to : to + rows] = pieces[g][at + h * head : at + (h + 1) * head, :]
    for h in range(heads):
        v_all[h, head:, :] = jnp.ones((EXTRA, v_all.shape[2]), jnp.bfloat16)
    for first in range(0, len(biases), LANES):
        some = biases[first : first + LANES]
        fill = [jnp.zeros((LANES - len(some), LANES), jnp.float32)] if len(some) < LANES else []
        columns = jnp.concatenate(some + fill, axis=0).T
        for i in range(len(some)):
            to = (first + i) * rows
            b_all[to : to + rows, :] = jnp.broadcast_to(columns[:, i : i + 1], (rows, LANES))
    for slot in range(WAYS):
        q_all[slot * rows : (slot + 1) * rows, :] = queries[slot][...]
    lane = lax.broadcasted_iota(jnp.int32, (1, width), 1)
    span = 2 * rows

    def one_block(index, _):
        query = q_all[pl.ds(pl.multiple_of(index * span, span), span), :]
        columns = []
        for h in range(heads):
            inside = (lane >= h * head) & (lane < (h + 1) * head)
            masked = jnp.where(inside, query, jnp.zeros_like(query))
            scores = lax.dot_general(k_all[...], masked, (((1,), (1,)), ((), ())), preferred_element_type=jnp.float32)
            bias = b_all[...]
            scores = scores + jnp.concatenate([bias] * (span // LANES), axis=-1)
            highest = jnp.max(scores, axis=0, keepdims=True)
            expo = jnp.exp(scores - highest).astype(jnp.bfloat16)
            numer = jnp.dot(v_all[h], expo, preferred_element_type=jnp.float32)
            at = h * deep
            if earlier:
                highest_before = before[index, at + head + 8 : at + head + 9, :]
                most = jnp.maximum(highest, highest_before)
                now, then = jnp.exp(highest - most), jnp.exp(highest_before - most)
                total = numer[head : head + 1, :] * now + before[index, at + head : at + head + 1, :] * then
                both = numer[:head, :] * now + before[index, at : at + head, :] * then
                columns.append(both / total)
            else:
                o_all[index, at : at + head + 8, :] = numer[: head + 8, :]
                o_all[index, at + head + 8 : at + deep, :] = jnp.broadcast_to(highest, (deep - head - 8, span))
        if earlier:
            o_all[index] = jnp.concatenate(columns, axis=0)
        return 0

    lax.fori_loop(0, WAYS // 2, one_block, 0)
    if earlier:
        for slot in range(WAYS):
            at = (slot % 2) * rows
            outs[slot][...] = o_all[slot // 2, :, at : at + rows].T.astype(jnp.bfloat16)


def half_of(half):
    spare = half % LANES
    span = half + spare
    return spare, span, pl.multiple_of(lax.axis_index("cfg") * (half - spare), LANES)


def fetch_kernel(w_ref, out_ref, sem):
    _, span, start = half_of(w_ref.shape[1] // 2)
    copy = pltpu.make_async_copy(w_ref.at[:, pl.ds(start, span)], out_ref, sem)
    copy.start()
    copy.wait()


def project(pieces, w_ref, way):
    rows, width = pieces[0].shape
    total = jnp.zeros((rows, w_ref.shape[1]), jnp.float32)
    for slot, piece in enumerate(pieces):
        w = w_ref[pl.ds(pl.multiple_of((way ^ slot) * width, width), width), :]
        total += jnp.dot(piece[...], w, preferred_element_type=jnp.float32)
    return total


def own_kernel(*refs, groups):
    *pieces, w_ref, out_ref = refs
    out_ref[...] = project(pieces, w_ref, lax.axis_index("seq") // groups)


def final_kernel(block_ref, *refs, groups, half):
    *pieces, own_ref, w_ref, modulation_ref, out_ref = refs
    spare, span, start = half_of(half)
    total = project(pieces, w_ref, lax.axis_index("seq") // groups)
    is_text = text_rows(block_ref[0], total.shape[0])
    table = modulation_ref[:, pl.ds(start, span)]
    gate = jnp.where(is_text, table[5:6, :], table[2:3, :])
    other = gate * total
    own = gate * own_ref[...]
    is_first = lax.axis_index("cfg") == 0
    cond = jnp.where(is_first, own, other)
    uncond = jnp.where(is_first, other, own)
    guided = (uncond + GUIDANCE * (cond - uncond)).T
    out_ref[...] = jnp.where(is_first, guided[:half, :], guided[spare:, :])


def block(hidden, modulation, w_qkv, q_gain, k_gain, w_out, text_count, block_order):
    states = hidden[0]
    rows, features = states.shape
    head = q_gain.shape[0]
    inner = w_qkv.shape[2]
    width = inner // WAYS
    count = lax.axis_size("seq")
    groups = count // WAYS
    bf16 = jnp.bfloat16
    smem = pl.BlockSpec(memory_space=pltpu.SMEM)
    vmem = pl.BlockSpec(memory_space=pltpu.VMEM)
    hbm = pl.BlockSpec(memory_space=pltpu.HBM)

    def limit(mib):
        return pltpu.CompilerParams(vmem_limit_bytes=min(mib, 60) * 2**20)

    w_qkv, w_out, states, modulation = (
        pltpu.with_memory_space_constraint(x, pltpu.HBM) for x in (w_qkv, w_out, states, modulation)
    )
    held_in = functools.partial(pltpu.with_memory_space_constraint, memory_space=pltpu.VMEM)

    def exchange(x, bits):
        return lax.ppermute(x, "seq", [(i, i ^ bits) for i in range(count)])

    def spread(slots):
        far = {s: exchange(slots[s], s * groups) for s in reversed(range(1, WAYS))}
        return [slots[0]] + [far[s] for s in range(1, WAYS)]

    size = (width // LANES) * rows + EXTRA + width
    kv_piece = pltpu.VMEM((size, LANES), bf16)
    piece = pltpu.VMEM((rows, width), bf16)
    *kv_slots, modded = pl.pallas_call(
        functools.partial(key_value_kernel, head=head, groups=groups),
        compiler_params=limit(16),
        in_specs=[smem, smem, hbm, hbm, hbm, vmem],
        out_shape=[kv_piece] * WAYS + [pltpu.VMEM((rows, features), bf16)],
        scratch_shapes=[
            pltpu.VMEM((rows, features), bf16),
            pltpu.VMEM(modulation.shape, jnp.float32),
            pltpu.VMEM((2, features, inner), bf16),
            pltpu.SemaphoreType.DMA((4,)),
        ],
    )(block_order, text_count, states, modulation, w_qkv, k_gain[None, :])
    kv = spread(kv_slots)
    q_slots = pl.pallas_call(
        functools.partial(query_kernel, head=head, groups=groups),
        compiler_params=limit(10),
        in_specs=[vmem, hbm, vmem],
        out_shape=[piece] * WAYS,
        scratch_shapes=[pltpu.VMEM((features, inner), bf16), pltpu.SemaphoreType.DMA],
    )(held_in(modded), w_qkv, q_gain[None, :])
    queries = spread(q_slots)
    half = w_out.shape[1] // 2
    span = half + half % LANES
    w_half = pl.pallas_call(
        fetch_kernel,
        compiler_params=limit(2),
        in_specs=[hbm],
        out_shape=pltpu.VMEM((inner, span), bf16),
        scratch_shapes=[pltpu.SemaphoreType.DMA],
    )(w_out)
    top = groups // 2

    def gathered(held):
        bit = top // 2
        while bit:
            held = held + [exchange(x, bit) for x in held]
            bit //= 2
        return held

    near = gathered(kv)
    order = [0, 1, 3, 2]
    crossed = {i: exchange(kv[i], top) for i in order}
    far = gathered([crossed[i] for i in order])
    keys = count * rows // 2
    deep = head + EXTRA
    roomy = count * rows <= 4096

    def attend(pieces, before, out_shape, scratch):
        ins = [held_in(x) if roomy else x for x in [*queries, *pieces]] + before
        return pl.pallas_call(
            functools.partial(attention_kernel, held=len(pieces), head=head, earlier=bool(before)),
            compiler_params=limit(8 + keys // 96),
            in_specs=[vmem] * len(ins),
            out_shape=out_shape,
            scratch_shapes=[
                pltpu.VMEM((keys, width), bf16),
                pltpu.VMEM((width // head, deep, keys), bf16),
                pltpu.VMEM((keys, LANES), jnp.float32),
                pltpu.VMEM((WAYS * rows, width), bf16),
            ]
            + scratch,
        )(*ins)

    part = pltpu.VMEM((WAYS // 2, deep * (width // head), 2 * rows), jnp.float32)
    before = attend(near, [], part, [])
    merged = pltpu.VMEM((WAYS // 2, width, 2 * rows), jnp.float32)
    o_slots = attend(far, [held_in(before)], [piece] * WAYS, [merged])
    attended = spread(o_slots)
    cfg_count = lax.axis_size("cfg")
    partner = []
    for x in attended:
        partner.append(lax.ppermute(x, "cfg", [(j, j ^ 1) for j in range(cfg_count)]))
    own = pl.pallas_call(
        functools.partial(own_kernel, groups=groups),
        compiler_params=limit(6),
        in_specs=[vmem] * (WAYS + 1),
        out_shape=pltpu.VMEM((rows, span), jnp.float32),
    )(*map(held_in, attended), held_in(w_half))
    guided = pl.pallas_call(
        functools.partial(final_kernel, groups=groups, half=half),
        compiler_params=limit(8),
        in_specs=[smem] + [vmem] * (WAYS + 3),
        out_shape=jax.ShapeDtypeStruct((half, rows), jnp.float32),
    )(block_order, *map(held_in, partner), held_in(own), held_in(w_half), modulation)
    return guided.T


def solution(mesh):
    in_specs = (P("cfg", "seq", None), P(), P(), P(), P(), P(), P("cfg"), P("seq"))
    out_specs = P("seq", "cfg")
    return jax.shard_map(block, mesh=mesh, in_specs=in_specs, out_specs=out_specs, check_vma=False)
```

```python
import functools

import jax
import jax.numpy as jnp
from jax import lax
from jax.experimental import pallas as pl
from jax.experimental.pallas import tpu as pltpu
from jax.sharding import PartitionSpec as P


TXT = 226
GUIDANCE = 6.0
EPSILON = 1e-05
MASKED = -1000000000.0
WAYS = 4
LANES = 128
EXTRA = 16


def text_rows(block, rows):
    within = lax.broadcasted_iota(jnp.int32, (rows, 1), 0)
    return block * rows + within < TXT


def modulate(block, states, modulation_ref):
    average = jnp.mean(states, axis=-1, keepdims=True)
    centred = states - average
    spread = jnp.mean(centred * centred, axis=-1, keepdims=True)
    normed = centred * lax.rsqrt(spread + EPSILON)
    is_text = text_rows(block, states.shape[0])
    table = modulation_ref[...]
    shift = jnp.where(is_text, table[3:4, :], table[0:1, :])
    scale = jnp.where(is_text, table[4:5, :], table[1:2, :])
    return (normed * (1.0 + scale) + shift).astype(jnp.bfloat16)


def head_normal(tile, gain, head):
    lane = lax.broadcasted_iota(jnp.int32, (1, LANES), 1)

    def average(x):
        mean = jnp.zeros(x.shape, jnp.float32)
        for first in range(0, LANES, head):
            inside = (lane >= first) & (lane < first + head)
            total = jnp.sum(jnp.where(inside, x, 0.0), axis=-1, keepdims=True)
            mean = jnp.where(inside, total * (1.0 / head), mean)
        return mean

    centred = tile - average(tile)
    return centred * lax.rsqrt(average(centred * centred) + EPSILON) * gain


def wide(gain):
    return jnp.concatenate([gain] * (LANES // gain.shape[1]), axis=-1)


def key_value_kernel(block_ref, count_ref, hidden_ref, modulation_ref, w_ref, gain_ref, *refs, head, groups):
    slots, (modded_ref, states, table, w_all, sems) = refs[:WAYS], refs[WAYS:]
    first = [
        pltpu.make_async_copy(hidden_ref, states, sems.at[2]),
        pltpu.make_async_copy(modulation_ref, table, sems.at[3]),
    ]
    copies = [pltpu.make_async_copy(w_ref.at[1 + i], w_all.at[i], sems.at[i]) for i in range(2)]
    for copy in first + copies:
        copy.start()
    for copy in first:
        copy.wait()
    block = block_ref[0]
    modded_ref[...] = modulate(block, states[...].astype(jnp.float32), table)
    rows = modded_ref.shape[0]
    width = w_all.shape[2] // WAYS
    gain = wide(gain_ref[...])
    way = lax.axis_index("seq") // groups
    position = block * rows + lax.broadcasted_iota(jnp.int32, (EXTRA, rows), 1)
    keep = (position >= TXT) | (position < count_ref[0])
    bias = jnp.where(keep, 0.0, MASKED).astype(jnp.bfloat16)
    starts = [pl.multiple_of((way ^ slot) * width, width) for slot in range(WAYS)]
    copies[0].wait()
    for slot in range(WAYS):
        w = w_all[0, :, pl.ds(starts[slot], width)]
        keys = jnp.dot(modded_ref[...], w, preferred_element_type=jnp.float32)
        for tile in range(width // LANES):
            normed = head_normal(keys[:, tile * LANES : (tile + 1) * LANES], gain, head)
            slots[slot][tile * rows : (tile + 1) * rows, :] = normed.astype(jnp.bfloat16)
        at = rows * (width // LANES)
        slots[slot][at : at + EXTRA, :] = bias
    copies[1].wait()
    for slot in range(WAYS):
        w = w_all[1, :, pl.ds(starts[slot], width)]
        values = jnp.dot(modded_ref[...], w, preferred_element_type=jnp.float32)
        slots[slot][at + EXTRA :, :] = values.T.astype(jnp.bfloat16)


def query_kernel(modded_ref, w_ref, gain_ref, *refs, head, groups):
    slots, (w_all, sem) = refs[:WAYS], refs[WAYS:]
    copy = pltpu.make_async_copy(w_ref.at[0], w_all, sem)
    copy.start()
    width = w_all.shape[1] // WAYS
    gain = wide(gain_ref[...])
    way = lax.axis_index("seq") // groups
    copy.wait()
    for slot in range(WAYS):
        start = pl.multiple_of((way ^ slot) * width, width)
        query = jnp.dot(modded_ref[...], w_all[:, pl.ds(start, width)], preferred_element_type=jnp.float32)
        for tile in range(width // LANES):
            at = slice(tile * LANES, (tile + 1) * LANES)
            normed = head_normal(query[:, at], gain, head).astype(jnp.bfloat16)
            slots[slot][at, :] = (normed * jnp.asarray(head ** (-0.5), jnp.bfloat16)).T


def attention_kernel(*refs, held, head, earlier):
    queries, refs = refs[:WAYS], refs[WAYS:]
    pieces, refs = refs[:held], refs[held:]
    if earlier:
        before, *outs, k_all, v_all, b_all, s_all, o_all = refs
    else:
        o_all, k_all, v_all, b_all, s_all = refs
    width, rows = queries[0].shape
    heads = width // head
    tiles = width // LANES
    deep = head + EXTRA
    size = tiles * rows + EXTRA + width
    biases = []
    for g in range(held):
        for p in range(pieces[g].shape[0] // size):
            to, at = len(biases) * rows, p * size
            for tile in range(tiles):
                k_all[to : to + rows, tile * LANES : (tile + 1) * LANES] = pieces[g][at + tile * rows : at + (tile + 1) * rows, :]
            at += tiles * rows
            biases.append(pieces[g][at : at + EXTRA, :].astype(jnp.float32)[0:1, :])
            at += EXTRA
            for h in range(heads):
                v_all[h, :head, to : to + rows] = pieces[g][at + h * head : at + (h + 1) * head, :]
    for h in range(heads):
        v_all[h, head:, :] = jnp.ones((EXTRA, v_all.shape[2]), jnp.bfloat16)
    for first in range(0, len(biases), LANES):
        some = biases[first : first + LANES]
        fill = [jnp.zeros((LANES - len(some), LANES), jnp.float32)] if len(some) < LANES else []
        columns = jnp.concatenate(some + fill, axis=0).T
        for i in range(len(some)):
            to = (first + i) * rows
            b_all[to : to + rows, :] = jnp.broadcast_to(columns[:, i : i + 1], (rows, LANES))
    span = 2 * rows
    chunk = 2 * rows
    chunks = k_all.shape[0] // chunk
    steps = [(index, h) for index in range(WAYS // 2) for h in range(heads)]

    def one_head(step):
        index, h = steps[step]
        query = jnp.concatenate([queries[2 * index + i][h * head : (h + 1) * head, :] for i in range(2)], axis=1)
        sides = [jnp.zeros((n * head, span), jnp.bfloat16) for n in (h, heads - 1 - h)]
        return jnp.concatenate([x for x in (sides[0], query, sides[1]) if x.shape[0]], axis=0)

    def score(step, at, query, highest):
        scores = jnp.dot(k_all[at : at + chunk, :], query, preferred_element_type=jnp.float32)
        scores = scores + jnp.concatenate([b_all[at : at + chunk, :]] * (span // LANES), axis=-1)
        s_all[step % 2, at : at + chunk, :] = scores
        most = jnp.max(scores, axis=0, keepdims=True)
        return most if highest is None else jnp.maximum(highest, most)

    def finish(step, highest, numer):
        index, h = steps[step]
        at = h * deep
        if earlier:
            highest_before = before[index, at + head + 8 : at + head + 9, :]
            most = jnp.maximum(highest, highest_before)
            now, then = jnp.exp(highest - most), jnp.exp(highest_before - most)
            total = numer[head : head + 1, :] * now + before[index, at + head : at + head + 1, :] * then
            both = numer[:head, :] * now + before[index, at : at + head, :] * then
            o_all[index, h * head : (h + 1) * head, :] = both / total
        else:
            o_all[index, at : at + head + 8, :] = numer[: head + 8, :]
            o_all[index, at + head + 8 : at + deep, :] = jnp.broadcast_to(highest, (deep - head - 8, span))

    highest = None
    for step in range(len(steps) + 1):
        ready, highest = highest, None
        query = one_head(step) if step < len(steps) else None
        numer = jnp.zeros((deep, span), jnp.float32)
        for c in range(chunks):
            at = c * chunk
            if query is not None:
                highest = score(step, at, query, highest)
            if step:
                expo = jnp.exp(s_all[(step - 1) % 2, at : at + chunk, :] - ready).astype(jnp.bfloat16)
                values = v_all[steps[step - 1][1], :, at : at + chunk]
                numer += jnp.dot(values, expo, preferred_element_type=jnp.float32)
        if step:
            finish(step - 1, ready, numer)
    if earlier:
        for slot in range(WAYS):
            at = (slot % 2) * rows
            outs[slot][...] = o_all[slot // 2, :, at : at + rows].T.astype(jnp.bfloat16)


def half_of(half):
    spare = half % LANES
    span = half + spare
    return spare, span, pl.multiple_of(lax.axis_index("cfg") * (half - spare), LANES)


def fetch_kernel(w_ref, out_ref, sem):
    _, span, start = half_of(w_ref.shape[1] // 2)
    copy = pltpu.make_async_copy(w_ref.at[:, pl.ds(start, span)], out_ref, sem)
    copy.start()
    copy.wait()


def project(pieces, w_ref, way):
    rows, width = pieces[0].shape
    total = jnp.zeros((rows, w_ref.shape[1]), jnp.float32)
    for slot, piece in enumerate(pieces):
        w = w_ref[pl.ds(pl.multiple_of((way ^ slot) * width, width), width), :]
        total += jnp.dot(piece[...], w, preferred_element_type=jnp.float32)
    return total


def own_kernel(*refs, groups):
    *pieces, w_ref, out_ref = refs
    out_ref[...] = project(pieces, w_ref, lax.axis_index("seq") // groups)


def final_kernel(block_ref, *refs, groups, half):
    *pieces, own_ref, w_ref, modulation_ref, out_ref = refs
    spare, span, start = half_of(half)
    total = project(pieces, w_ref, lax.axis_index("seq") // groups)
    is_text = text_rows(block_ref[0], total.shape[0])
    table = modulation_ref[:, pl.ds(start, span)]
    gate = jnp.where(is_text, table[5:6, :], table[2:3, :])
    other = gate * total
    own = gate * own_ref[...]
    is_first = lax.axis_index("cfg") == 0
    cond = jnp.where(is_first, own, other)
    uncond = jnp.where(is_first, other, own)
    guided = (uncond + GUIDANCE * (cond - uncond)).T
    out_ref[...] = jnp.where(is_first, guided[:half, :], guided[spare:, :])


def block(hidden, modulation, w_qkv, q_gain, k_gain, w_out, text_count, block_order):
    states = hidden[0]
    rows, features = states.shape
    head = q_gain.shape[0]
    inner = w_qkv.shape[2]
    width = inner // WAYS
    count = lax.axis_size("seq")
    groups = count // WAYS
    bf16 = jnp.bfloat16
    smem = pl.BlockSpec(memory_space=pltpu.SMEM)
    vmem = pl.BlockSpec(memory_space=pltpu.VMEM)
    hbm = pl.BlockSpec(memory_space=pltpu.HBM)

    def limit(mib):
        return pltpu.CompilerParams(vmem_limit_bytes=min(mib, 60) * 2**20)

    w_qkv, w_out, states, modulation = (
        pltpu.with_memory_space_constraint(x, pltpu.HBM) for x in (w_qkv, w_out, states, modulation)
    )
    held_in = functools.partial(pltpu.with_memory_space_constraint, memory_space=pltpu.VMEM)

    def exchange(x, bits):
        return lax.ppermute(x, "seq", [(i, i ^ bits) for i in range(count)])

    def spread(slots):
        far = {s: exchange(slots[s], s * groups) for s in reversed(range(1, WAYS))}
        return [slots[0]] + [far[s] for s in range(1, WAYS)]

    size = (width // LANES) * rows + EXTRA + width
    kv_piece = pltpu.VMEM((size, LANES), bf16)
    piece = pltpu.VMEM((rows, width), bf16)
    *kv_slots, modded = pl.pallas_call(
        functools.partial(key_value_kernel, head=head, groups=groups),
        compiler_params=limit(16),
        in_specs=[smem, smem, hbm, hbm, hbm, vmem],
        out_shape=[kv_piece] * WAYS + [pltpu.VMEM((rows, features), bf16)],
        scratch_shapes=[
            pltpu.VMEM((rows, features), bf16),
            pltpu.VMEM(modulation.shape, jnp.float32),
            pltpu.VMEM((2, features, inner), bf16),
            pltpu.SemaphoreType.DMA((4,)),
        ],
    )(block_order, text_count, states, modulation, w_qkv, k_gain[None, :])
    kv = spread(kv_slots)
    q_slots = pl.pallas_call(
        functools.partial(query_kernel, head=head, groups=groups),
        compiler_params=limit(10),
        in_specs=[vmem, hbm, vmem],
        out_shape=[pltpu.VMEM((width, rows), bf16)] * WAYS,
        scratch_shapes=[pltpu.VMEM((features, inner), bf16), pltpu.SemaphoreType.DMA],
    )(held_in(modded), w_qkv, q_gain[None, :])
    queries = spread(q_slots)
    half = w_out.shape[1] // 2
    span = half + half % LANES
    w_half = pl.pallas_call(
        fetch_kernel,
        compiler_params=limit(2),
        in_specs=[hbm],
        out_shape=pltpu.VMEM((inner, span), bf16),
        scratch_shapes=[pltpu.SemaphoreType.DMA],
    )(w_out)
    top = groups // 2

    def gathered(held):
        bit = top // 2
        while bit:
            held = held + [exchange(x, bit) for x in held]
            bit //= 2
        return held

    near = gathered(kv)
    order = [0, 1, 3, 2]
    crossed = {i: exchange(kv[i], top) for i in order}
    far = gathered([crossed[i] for i in order])
    keys = count * rows // 2
    deep = head + EXTRA
    roomy = count * rows <= 4096

    def attend(pieces, before, out_shape, scratch):
        ins = [held_in(x) if roomy else x for x in [*queries, *pieces]] + before
        return pl.pallas_call(
            functools.partial(attention_kernel, held=len(pieces), head=head, earlier=bool(before)),
            compiler_params=limit(8 + keys // 96),
            in_specs=[vmem] * len(ins),
            out_shape=out_shape,
            scratch_shapes=[
                pltpu.VMEM((keys, width), bf16),
                pltpu.VMEM((width // head, deep, keys), bf16),
                pltpu.VMEM((keys, LANES), jnp.float32),
                pltpu.VMEM((2, keys, 2 * rows), jnp.float32),
            ]
            + scratch,
        )(*ins)

    part = pltpu.VMEM((WAYS // 2, deep * (width // head), 2 * rows), jnp.float32)
    before = attend(near, [], part, [])
    merged = pltpu.VMEM((WAYS // 2, width, 2 * rows), jnp.float32)
    o_slots = attend(far, [held_in(before)], [piece] * WAYS, [merged])
    attended = spread(o_slots)
    cfg_count = lax.axis_size("cfg")
    partner = []
    for x in attended:
        partner.append(lax.ppermute(x, "cfg", [(j, j ^ 1) for j in range(cfg_count)]))
    own = pl.pallas_call(
        functools.partial(own_kernel, groups=groups),
        compiler_params=limit(6),
        in_specs=[vmem] * (WAYS + 1),
        out_shape=pltpu.VMEM((rows, span), jnp.float32),
    )(*map(held_in, attended), held_in(w_half))
    guided = pl.pallas_call(
        functools.partial(final_kernel, groups=groups, half=half),
        compiler_params=limit(8),
        in_specs=[smem] + [vmem] * (WAYS + 3),
        out_shape=jax.ShapeDtypeStruct((half, rows), jnp.float32),
    )(block_order, *map(held_in, partner), held_in(own), held_in(w_half), modulation)
    return guided.T


def solution(mesh):
    in_specs = (P("cfg", "seq", None), P(), P(), P(), P(), P(), P("cfg"), P("seq"))
    out_specs = P("seq", "cfg")
    return jax.shard_map(block, mesh=mesh, in_specs=in_specs, out_specs=out_specs, check_vma=False)
```

```python
import functools

import jax
import jax.numpy as jnp
from jax import lax
from jax.experimental import pallas as pl
from jax.experimental.pallas import tpu as pltpu
from jax.sharding import PartitionSpec as P


TXT = 226
GUIDANCE = 6.0
EPSILON = 1e-05
MASKED = -1000000000.0
WAYS = 4
LANES = 128
EXTRA = 16


def text_rows(block, rows):
    within = lax.broadcasted_iota(jnp.int32, (rows, 1), 0)
    return block * rows + within < TXT


def modulate(block, states, modulation_ref):
    average = jnp.mean(states, axis=-1, keepdims=True)
    centred = states - average
    spread = jnp.mean(centred * centred, axis=-1, keepdims=True)
    normed = centred * lax.rsqrt(spread + EPSILON)
    is_text = text_rows(block, states.shape[0])
    table = modulation_ref[...]
    shift = jnp.where(is_text, table[3:4, :], table[0:1, :])
    scale = jnp.where(is_text, table[4:5, :], table[1:2, :])
    return (normed * (1.0 + scale) + shift).astype(jnp.bfloat16)


def head_normal(tile, gain, head):
    lane = lax.broadcasted_iota(jnp.int32, (1, LANES), 1)

    def average(x):
        mean = jnp.zeros(x.shape, jnp.float32)
        for first in range(0, LANES, head):
            inside = (lane >= first) & (lane < first + head)
            total = jnp.sum(jnp.where(inside, x, 0.0), axis=-1, keepdims=True)
            mean = jnp.where(inside, total * (1.0 / head), mean)
        return mean

    centred = tile - average(tile)
    return centred * lax.rsqrt(average(centred * centred) + EPSILON) * gain


def wide(gain):
    return jnp.concatenate([gain] * (LANES // gain.shape[1]), axis=-1)


def key_value_kernel(block_ref, count_ref, hidden_ref, modulation_ref, w_ref, gain_ref, *refs, head, groups):
    slots, (modded_ref, states, table, gains, w_all, sems) = refs[:WAYS], refs[WAYS:]
    first = [
        pltpu.make_async_copy(hidden_ref, states, sems.at[2]),
        pltpu.make_async_copy(modulation_ref, table, sems.at[3]),
        pltpu.make_async_copy(gain_ref, gains, sems.at[4]),
    ]
    copies = [pltpu.make_async_copy(w_ref.at[1 + i], w_all.at[i], sems.at[i]) for i in range(2)]
    for copy in first + copies:
        copy.start()
    for copy in first:
        copy.wait()
    block = block_ref[0]
    modded_ref[...] = modulate(block, states[...].astype(jnp.float32), table)
    rows = modded_ref.shape[0]
    width = w_all.shape[2] // WAYS
    gain = wide(gains[...])
    way = lax.axis_index("seq") // groups
    position = block * rows + lax.broadcasted_iota(jnp.int32, (EXTRA, rows), 1)
    keep = (position >= TXT) | (position < count_ref[0])
    bias = jnp.where(keep, 0.0, MASKED).astype(jnp.bfloat16)
    starts = [pl.multiple_of((way ^ slot) * width, width) for slot in range(WAYS)]
    copies[0].wait()
    for slot in range(WAYS):
        w = w_all[0, :, pl.ds(starts[slot], width)]
        keys = jnp.dot(modded_ref[...], w, preferred_element_type=jnp.float32)
        for tile in range(width // LANES):
            normed = head_normal(keys[:, tile * LANES : (tile + 1) * LANES], gain, head)
            slots[slot][tile * rows : (tile + 1) * rows, :] = normed.astype(jnp.bfloat16)
        at = rows * (width // LANES)
        slots[slot][at : at + EXTRA, :] = bias
    copies[1].wait()
    for slot in range(WAYS):
        w = w_all[1, :, pl.ds(starts[slot], width)]
        values = jnp.dot(modded_ref[...], w, preferred_element_type=jnp.float32)
        slots[slot][at + EXTRA :, :] = values.T.astype(jnp.bfloat16)


def query_kernel(modded_ref, w_ref, gain_ref, *refs, head, groups):
    slots, (gains, w_all, sems) = refs[:WAYS], refs[WAYS:]
    copy = pltpu.make_async_copy(w_ref.at[0], w_all, sems.at[0])
    copy.start()
    small = pltpu.make_async_copy(gain_ref, gains, sems.at[1])
    small.start()
    small.wait()
    width = w_all.shape[1] // WAYS
    gain = wide(gains[...])
    way = lax.axis_index("seq") // groups
    copy.wait()
    for slot in range(WAYS):
        start = pl.multiple_of((way ^ slot) * width, width)
        query = jnp.dot(modded_ref[...], w_all[:, pl.ds(start, width)], preferred_element_type=jnp.float32)
        for tile in range(width // LANES):
            at = slice(tile * LANES, (tile + 1) * LANES)
            normed = head_normal(query[:, at], gain, head).astype(jnp.bfloat16)
            slots[slot][at, :] = (normed * jnp.asarray(head ** (-0.5), jnp.bfloat16)).T


def attention_kernel(*refs, queries, held, outs, head, earlier):
    queries, refs = refs[:queries], refs[queries:]
    pieces, refs = refs[:held], refs[held:]
    if earlier is not None:
        before, refs = refs[0], refs[1:]
    if earlier is None:
        o_all, k_all, v_all, b_all, s_all = refs
    elif held:
        outs, (k_all, v_all, b_all, s_all, o_all) = refs[:outs], refs[outs:]
    else:
        (k_all, v_all, b_all), refs = refs[:3], refs[3:]
        outs, (s_all, o_all) = refs[:outs], refs[outs:]
    width, rows = queries[0].shape
    heads = width // head
    tiles = width // LANES
    deep = head + EXTRA
    size = tiles * rows + EXTRA + width
    biases = []
    for g in range(held):
        for p in range(pieces[g].shape[0] // size):
            to, at = len(biases) * rows, p * size
            for tile in range(tiles):
                k_all[to : to + rows, tile * LANES : (tile + 1) * LANES] = pieces[g][at + tile * rows : at + (tile + 1) * rows, :]
            at += tiles * rows
            biases.append(pieces[g][at : at + EXTRA, :].astype(jnp.float32)[0:1, :])
            at += EXTRA
            for h in range(heads):
                v_all[h, :head, to : to + rows] = pieces[g][at + h * head : at + (h + 1) * head, :]
    for h in range(heads if held else 0):
        v_all[h, head:, :] = jnp.ones((EXTRA, v_all.shape[2]), jnp.bfloat16)
    for first in range(0, len(biases), LANES):
        some = biases[first : first + LANES]
        fill = [jnp.zeros((LANES - len(some), LANES), jnp.float32)] if len(some) < LANES else []
        columns = jnp.concatenate(some + fill, axis=0).T
        for i in range(len(some)):
            to = (first + i) * rows
            b_all[to : to + rows, :] = jnp.broadcast_to(columns[:, i : i + 1], (rows, LANES))
    span = 2 * rows
    chunk = 2 * rows
    chunks = k_all.shape[0] // chunk
    steps = [(index, h) for index in range(len(queries) // 2) for h in range(heads)]

    def one_head(step):
        index, h = steps[step]
        query = jnp.concatenate([queries[2 * index + i][h * head : (h + 1) * head, :] for i in range(2)], axis=1)
        sides = [jnp.zeros((n * head, span), jnp.bfloat16) for n in (h, heads - 1 - h)]
        return jnp.concatenate([x for x in (sides[0], query, sides[1]) if x.shape[0]], axis=0)

    def score(step, at, query, highest):
        scores = jnp.dot(k_all[at : at + chunk, :], query, preferred_element_type=jnp.float32)
        scores = scores + jnp.concatenate([b_all[at : at + chunk, :]] * (span // LANES), axis=-1)
        s_all[step % 2, at : at + chunk, :] = scores
        most = jnp.max(scores, axis=0, keepdims=True)
        return most if highest is None else jnp.maximum(highest, most)

    def finish(step, highest, numer):
        index, h = steps[step]
        at = h * deep
        if earlier is not None:
            past = earlier + index
            highest_before = before[past, at + head + 8 : at + head + 9, :]
            most = jnp.maximum(highest, highest_before)
            now, then = jnp.exp(highest - most), jnp.exp(highest_before - most)
            total = numer[head : head + 1, :] * now + before[past, at + head : at + head + 1, :] * then
            both = numer[:head, :] * now + before[past, at : at + head, :] * then
            o_all[index, h * head : (h + 1) * head, :] = both / total
        else:
            o_all[index, at : at + head + 8, :] = numer[: head + 8, :]
            o_all[index, at + head + 8 : at + deep, :] = jnp.broadcast_to(highest, (deep - head - 8, span))

    highest = None
    for step in range(len(steps) + 1):
        ready, highest = highest, None
        query = one_head(step) if step < len(steps) else None
        numer = jnp.zeros((deep, span), jnp.float32)
        for c in range(chunks):
            at = c * chunk
            if query is not None:
                highest = score(step, at, query, highest)
            if step:
                expo = jnp.exp(s_all[(step - 1) % 2, at : at + chunk, :] - ready).astype(jnp.bfloat16)
                values = v_all[steps[step - 1][1], :, at : at + chunk]
                numer += jnp.dot(values, expo, preferred_element_type=jnp.float32)
        if step:
            finish(step - 1, ready, numer)
    if earlier is not None:
        for slot in range(len(queries)):
            at = (slot % 2) * rows
            outs[slot][...] = o_all[slot // 2, :, at : at + rows].T.astype(jnp.bfloat16)


def half_of(half):
    spare = half % LANES
    span = half + spare
    return spare, span, pl.multiple_of(lax.axis_index("cfg") * (half - spare), LANES)


def fetch_kernel(block_ref, w_ref, modulation_ref, out_ref, gate_ref, table, sems):
    _, span, start = half_of(w_ref.shape[1] // 2)
    small = pltpu.make_async_copy(modulation_ref, table, sems.at[0])
    copy = pltpu.make_async_copy(w_ref.at[:, pl.ds(start, span)], out_ref, sems.at[1])
    small.start()
    copy.start()
    small.wait()
    is_text = text_rows(block_ref[0], gate_ref.shape[0])
    gates = table[:, pl.ds(start, span)]
    gate_ref[...] = jnp.where(is_text, gates[5:6, :], gates[2:3, :])
    copy.wait()


def project(pieces, w_ref, way):
    rows, width = pieces[0].shape
    total = jnp.zeros((rows, w_ref.shape[1]), jnp.float32)
    for slot, piece in enumerate(pieces):
        w = w_ref[pl.ds(pl.multiple_of((way ^ slot) * width, width), width), :]
        total += jnp.dot(piece[...], w, preferred_element_type=jnp.float32)
    return total


def own_kernel(*refs, groups):
    *pieces, gate_ref, w_ref, out_ref = refs
    out_ref[...] = gate_ref[...] * project(pieces, w_ref, lax.axis_index("seq") // groups)


def final_kernel(*refs, groups, half):
    *pieces, own_ref, gate_ref, w_ref, out_ref = refs
    spare = half_of(half)[0]
    other = gate_ref[...] * project(pieces, w_ref, lax.axis_index("seq") // groups)
    own = own_ref[...]
    is_first = lax.axis_index("cfg") == 0
    cond = jnp.where(is_first, own, other)
    uncond = jnp.where(is_first, other, own)
    guided = (uncond + GUIDANCE * (cond - uncond)).T
    out_ref[...] = jnp.where(is_first, guided[:half, :], guided[spare:, :])


def block(hidden, modulation, w_qkv, q_gain, k_gain, w_out, text_count, block_order):
    states = hidden[0]
    rows, features = states.shape
    head = q_gain.shape[0]
    inner = w_qkv.shape[2]
    width = inner // WAYS
    count = lax.axis_size("seq")
    groups = count // WAYS
    bf16 = jnp.bfloat16
    smem = pl.BlockSpec(memory_space=pltpu.SMEM)
    vmem = pl.BlockSpec(memory_space=pltpu.VMEM)
    hbm = pl.BlockSpec(memory_space=pltpu.HBM)

    def limit(mib):
        return pltpu.CompilerParams(vmem_limit_bytes=min(mib, 60) * 2**20)

    in_hbm = functools.partial(pltpu.with_memory_space_constraint, memory_space=pltpu.HBM)
    w_qkv, w_out, states, modulation = map(in_hbm, (w_qkv, w_out, states, modulation))
    held_in = functools.partial(pltpu.with_memory_space_constraint, memory_space=pltpu.VMEM)

    def exchange(x, bits):
        return lax.ppermute(x, "seq", [(i, i ^ bits) for i in range(count)])

    def spread(slots):
        far = {s: exchange(slots[s], s * groups) for s in reversed(range(1, WAYS))}
        return [slots[0]] + [far[s] for s in range(1, WAYS)]

    size = (width // LANES) * rows + EXTRA + width
    kv_piece = pltpu.VMEM((size, LANES), bf16)
    piece = pltpu.VMEM((rows, width), bf16)
    *kv_slots, modded = pl.pallas_call(
        functools.partial(key_value_kernel, head=head, groups=groups),
        compiler_params=limit(16),
        in_specs=[smem, smem, hbm, hbm, hbm, hbm],
        out_shape=[kv_piece] * WAYS + [pltpu.VMEM((rows, features), bf16)],
        scratch_shapes=[
            pltpu.VMEM((rows, features), bf16),
            pltpu.VMEM(modulation.shape, jnp.float32),
            pltpu.VMEM((1, head), jnp.float32),
            pltpu.VMEM((2, features, inner), bf16),
            pltpu.SemaphoreType.DMA((5,)),
        ],
    )(block_order, text_count, states, modulation, w_qkv, in_hbm(k_gain[None, :]))
    kv = spread(kv_slots)
    q_slots = pl.pallas_call(
        functools.partial(query_kernel, head=head, groups=groups),
        compiler_params=limit(10),
        in_specs=[vmem, hbm, hbm],
        out_shape=[pltpu.VMEM((width, rows), bf16)] * WAYS,
        scratch_shapes=[
            pltpu.VMEM((1, head), jnp.float32),
            pltpu.VMEM((features, inner), bf16),
            pltpu.SemaphoreType.DMA((2,)),
        ],
    )(held_in(modded), w_qkv, in_hbm(q_gain[None, :]))
    queries = spread(q_slots)
    half = w_out.shape[1] // 2
    span = half + half % LANES
    w_half, gate = pl.pallas_call(
        fetch_kernel,
        compiler_params=limit(3),
        in_specs=[smem, hbm, hbm],
        out_shape=[pltpu.VMEM((inner, span), bf16), pltpu.VMEM((rows, span), jnp.float32)],
        scratch_shapes=[pltpu.VMEM(modulation.shape, jnp.float32), pltpu.SemaphoreType.DMA((2,))],
    )(block_order, w_out, modulation)
    top = groups // 2

    def gathered(held):
        bit = top // 2
        while bit:
            held = held + [exchange(x, bit) for x in held]
            bit //= 2
        return held

    near = gathered(kv)
    order = [0, 1, 3, 2]
    crossed = {i: exchange(kv[i], top) for i in order}
    far = gathered([crossed[i] for i in order])
    keys = count * rows // 2
    deep = head + EXTRA
    roomy = count * rows <= 4096

    laid = [
        pltpu.VMEM((keys, width), bf16),
        pltpu.VMEM((width // head, deep, keys), bf16),
        pltpu.VMEM((keys, LANES), jnp.float32),
    ]
    scores = pltpu.VMEM((2, keys, 2 * rows), jnp.float32)

    def attend(slots, pieces, more, earlier, outs, out_shape, scratch):
        ins = [held_in(x) if roomy else x for x in [*slots, *pieces]] + more
        return pl.pallas_call(
            functools.partial(
                attention_kernel, queries=len(slots), held=len(pieces), outs=outs, head=head, earlier=earlier
            ),
            compiler_params=limit(8 + keys // 96),
            in_specs=[vmem] * len(ins),
            out_shape=out_shape,
            scratch_shapes=scratch,
        )(*ins)

    part = pltpu.VMEM((WAYS // 2, deep * (width // head), 2 * rows), jnp.float32)
    merged = pltpu.VMEM((1, width, 2 * rows), jnp.float32)
    before = held_in(attend(queries, near, [], None, 0, [part], laid + [scores])[0])
    *o_far, k_all, v_all, b_all = attend(
        queries[2:], far, [before], 1, 2, [piece] * 2 + laid, [scores, merged])
    o_near = attend(
        queries[:2], [], [before, held_in(k_all), held_in(v_all), held_in(b_all)], 0, 2, [piece] * 2, [scores, merged])
    attended = spread([*o_near, *o_far])
    cfg_count = lax.axis_size("cfg")
    partner = []
    for x in attended:
        partner.append(lax.ppermute(x, "cfg", [(j, j ^ 1) for j in range(cfg_count)]))
    own = pl.pallas_call(
        functools.partial(own_kernel, groups=groups),
        compiler_params=limit(6),
        in_specs=[vmem] * (WAYS + 2),
        out_shape=pltpu.VMEM((rows, span), jnp.float32),
    )(*map(held_in, [*attended, gate, w_half]))
    guided = pl.pallas_call(
        functools.partial(final_kernel, groups=groups, half=half),
        compiler_params=limit(8),
        in_specs=[vmem] * (WAYS + 3),
        out_shape=jax.ShapeDtypeStruct((half, rows), jnp.float32),
    )(*map(held_in, [*partner, own, gate, w_half]))
    return guided.T


def solution(mesh):
    in_specs = (P("cfg", "seq", None), P(), P(), P(), P(), P(), P("cfg"), P("seq"))
    out_specs = P("seq", "cfg")
    return jax.shard_map(block, mesh=mesh, in_specs=in_specs, out_specs=out_specs, check_vma=False)
```
